128 devices in a mesh: sub: 32 (over z, y, core), blk: 4 (over x).
Axes of the slice: x: 4, y: 4, z: 4, core: 2. Of those that a mesh axis runs over, the one named last changes fastest.
Arguments:
- initial_state: float32 [32, 64, 2048], P('sub', None, 'blk'), may hold values from -6 to 6
- source: bfloat16 [32, 8, 64, 2048], P('sub', None, None, 'blk'), may hold values from -6 to 6
- inverse_diag: float32 [32, 2048], P('sub', 'blk'), may hold values from 0.5 to 0.85
- inverse_off: bfloat16 [32, 2048, 2048], P('sub', None, 'blk'), may hold values from -0.032958984 to 0.032958984
- coupling: float32 [32, 128], P('sub', 'blk'), may hold values from 0.3 to 3
- initial_waves: bfloat16 [32, 128, 512], P('sub', 'blk'), may hold values from -6 to 6
- bucket: int32 [32], P('sub'), may hold values from 0 to 2
- partner: int32 [32, 128], P('sub', 'blk'), may hold values from 0 to 31
- position_of: int32 [32], replicated, may hold values from 0 to 31, each once
Outputs:
- last_state: float32 [32, 64, 2048], P('sub', None, 'blk')
- waveform: float32 [32, 128, 512], P('sub', 'blk')
The draws below stay inside these ranges and needn't reach their ends.
Inputs may be any that keep to these rules, and one draw needn't show every extreme that they name: A subcircuit of bucket b takes 8 / 2 ** (2 - b) implicit Euler steps. `position_of`: a permutation.
All inputs are finite; a program needn't handle non-finite values.
Results may differ from the reference program's by a relative error of at most 0.0052.
Values may be sent and summed in bfloat16 or wider, within the bound.
No kernel may reach another device: no remote copies, remote signals or barrier semaphores. Data moves between devices by JAX's collectives and lax.ppermute only.
A program may use at most 64 MiB of HBM per device.

```python
import math
import jax
import jax.numpy as jnp
from jax import lax

NODES = 2048
PORTS = 128
STEPS = 8
SWEEPS = 2
INPUT_CASES = 64
SUBS = 32


def place_ends(values, rng, low, high):
    index_at = [jax.random.randint(jax.random.fold_in(rng, axis), (), 0, length) for axis, length in enumerate(values.shape)]
    longest = values.shape.index(max(values.shape))
    neighbour = index_at[:longest] + [(index_at[longest] + 1) % values.shape[longest]] + index_at[longest + 1:]
    return values.at[tuple(index_at)].set(low).at[tuple(neighbour)].set(high)


def block_levels(stream_key, shape, pieces, smallest, high):
    loudness, own = 1.0, jax.random.fold_in(stream_key, 6)
    for axis_at, shards_of in pieces:
        draws = jnp.exp(jax.random.uniform(jax.random.fold_in(own, axis_at), (shards_of,), jnp.float32, smallest / len(pieces), high / len(pieces)))
        loudness = loudness * jnp.repeat(draws, shape[axis_at] // shards_of).reshape([-1 if axis == axis_at else 1 for axis in range(len(shape))])
    return loudness


def gaussian(rng, shape, width, limit, cuts=(), kind=jnp.bfloat16):
    drawn = jax.random.normal(rng, shape, jnp.float32) * width
    if len(cuts) > 0:
        drawn = block_levels(rng, shape, cuts, -0.22, 0.18) * drawn
    return jnp.clip(drawn, min=-limit, max=limit).astype(kind)


def setup_inputs(seed: int = 0) -> dict:
    streams_of = jax.random.split(jax.random.key(seed), 10)
    initial_state = gaussian(streams_of[0], (SUBS, INPUT_CASES, NODES), 1.0, 6.0, ((0, 32), (2, 4)), jnp.float32)
    source = gaussian(streams_of[1], (SUBS, STEPS, INPUT_CASES, NODES), 0.5, 6.0, ((0, 32), (3, 4)))
    inverse_diag = jnp.clip(0.5 + 0.35000002 * jax.random.uniform(streams_of[2], (SUBS, NODES), jnp.float32) ** block_levels(streams_of[2], (SUBS, NODES), ((0, 32), (1, 4)), -0.2, 0.2), 0.5, 0.85)
    inverse_off = gaussian(streams_of[3], (SUBS, NODES, NODES), (0.25 * NODES ** -0.5), 0.032958984, ((0, 32), (2, 4)))
    coupling = jnp.clip(jnp.exp(math.log(3.0) - 2.3025851 * jax.random.uniform(streams_of[4], (SUBS, PORTS), jnp.float32) ** block_levels(streams_of[4], (SUBS, PORTS), ((0, 32), (1, 4)), -0.2, 0.2)), 0.3, 3.0)
    initial_waves = gaussian(streams_of[5], (SUBS, PORTS, STEPS * INPUT_CASES), 1.0, 6.0, ((0, 32), (1, 4)))
    bucket = place_ends(jax.random.randint(streams_of[6], (SUBS,), 0, 3), jax.random.fold_in(streams_of[6], 1), 0, 2).astype(jnp.int32)
    partner = place_ends(jax.random.randint(streams_of[7], (SUBS, PORTS), 0, SUBS), jax.random.fold_in(streams_of[7], 1), 0, SUBS - 1).astype(jnp.int32)
    position_of = jax.random.permutation(streams_of[8], SUBS).astype(jnp.int32)
    return dict(initial_state=initial_state, source=source, inverse_diag=inverse_diag, inverse_off=inverse_off, coupling=coupling, initial_waves=initial_waves, bucket=bucket, partner=partner, position_of=position_of)


def step_count(bucket):
    return jnp.where(bucket == 0, STEPS // 4, jnp.where(bucket == 1, STEPS // 2, STEPS)).astype(jnp.int32)


def evolve(initial_state, source, inverse_diag, inverse_off, coupling, bucket, incoming):
    corners = initial_state.shape[0]
    stride = NODES // PORTS
    step_total = step_count(bucket)
    spacing = (STEPS // step_total).astype(jnp.int32)
    spacing_float = spacing.astype(jnp.float32)
    driven = incoming.astype(jnp.float32).reshape(PORTS, STEPS, corners)

    def advance(time_step_index, carried):
        current, sample_times = carried
        fine_index = ((time_step_index + 1) * spacing - 1).astype(jnp.int32)
        forcing = lax.dynamic_index_in_dim(source, fine_index, 0, keepdims=False).astype(jnp.float32)
        injected = coupling[:, None] * lax.dynamic_index_in_dim(driven, fine_index, 1, keepdims=False)
        spread = jnp.pad(injected.T[:, :, None], ((0, 0), (0, 0), (0, stride - 1))).reshape(corners, NODES)
        loop_argument = (current + spacing_float * (forcing + spread)).astype(jnp.bfloat16)
        loop_argument = lax.optimization_barrier(loop_argument)
        updated = inverse_diag[None, :] * loop_argument.astype(jnp.float32) + jnp.dot(loop_argument, inverse_off, preferred_element_type=jnp.float32)
        port_values = updated.reshape(corners, PORTS, stride)[:, :, 0]
        sample_times = lax.dynamic_update_index_in_dim(sample_times, port_values, time_step_index, 0)
        return updated, sample_times

    sample_times = jnp.zeros((STEPS, corners, PORTS), jnp.float32)
    last_state, sample_times = lax.fori_loop(0, step_total, advance, (initial_state, sample_times))
    held_index = jnp.arange(STEPS, dtype=jnp.int32) // spacing
    waveform = jnp.transpose(sample_times[held_index], (2, 0, 1)).reshape(PORTS, STEPS * corners)
    return last_state, waveform


def reference(initial_state, source, inverse_diag, inverse_off, coupling, initial_waves, bucket, partner, position_of):
    located = position_of[partner]
    port_index = jnp.arange(PORTS, dtype=jnp.int32)[None, :]
    waves = initial_waves
    for sweep_index in range(SWEEPS):
        incoming = waves[located, port_index]
        last_state, waveform = lax.map(lambda members: evolve(*members), (initial_state, source, inverse_diag, inverse_off, coupling, bucket, incoming))
        waves = waveform.astype(jnp.bfloat16)
    return last_state, waveform
```

```python
import functools

import jax
import jax.numpy as jnp
from jax import lax
from jax.experimental import pallas as pl
from jax.experimental.pallas import tpu as pltpu
from jax.sharding import PartitionSpec as P


F32 = jnp.float32
BF16 = jnp.bfloat16


def grid_of(mesh):
    subs, blks = mesh.shape["sub"], mesh.shape["blk"]
    return subs, blks


def move(array, mesh, target):
    subs, blks = grid_of(mesh)
    pairs = []
    for sub in range(subs):
        for x in range(blks):
            rel = (x - 2 * (sub % 2)) % blks
            to = target(x, rel)
            if to is not None:
                pairs.append((sub * blks + x, sub * blks + to % blks))
    return lax.ppermute(array, ("sub", "blk"), pairs)


def to_home(array, mesh):
    one = move(array, mesh, lambda x, rel: x - 1 if rel == 1 else None)
    two = move(array, mesh, lambda x, rel: x - 2 if rel == 2 else None)
    three = move(array, mesh, lambda x, rel: x + 1 if rel == 3 else None)
    return array, one, two, three


def from_home(slots, rel, mesh):
    one = move(slots[1], mesh, lambda x, r: x + 1 if r == 0 else None)
    two = move(slots[2], mesh, lambda x, r: x + 2 if r == 0 else None)
    three = move(slots[3], mesh, lambda x, r: x - 1 if r == 0 else None)
    return jnp.where(
        rel == 0, slots[0], jnp.where(rel == 1, one, jnp.where(rel == 2, two, three))
    )


def sweep_kernel(final, meta, a0, a1, a2t, a2b, a3, s0, s1, s2, s3, m0, m1, m2, m3,
                 w0, w1, w2, w3, out, operand, forced, history):
    steps, cases, block = s0.shape
    ports = w0.shape[0]
    slots = 4
    count, spacing, place = meta[0], meta[1], meta[2]
    spacing_float = spacing.astype(F32)
    sources, miscs = (s0, s1, s2, s3), (m0, m1, m2, m3)
    nodes = slots * block
    stride = block // ports
    waves = jnp.concatenate([w[...] for w in (w0, w1, w2, w3)], axis=0).astype(F32)
    waves = jnp.transpose(waves).astype(BF16)
    port_at = lax.broadcasted_iota(jnp.int32, (slots * ports, nodes), 0) * stride
    node_at = lax.broadcasted_iota(jnp.int32, (slots * ports, nodes), 1)
    spread = jnp.where(port_at == node_at, 1.0, 0.0).astype(BF16)
    forced[...] = jnp.dot(waves, spread, preferred_element_type=F32).astype(BF16)

    def step(k, current):
        fine = (k + 1) * spacing - 1
        rows = pl.ds(pl.multiple_of(fine * cases, cases), cases)
        for d in range(slots):
            lanes = slice(d * block, (d + 1) * block)
            drive = miscs[d][cases + 1 : cases + 2, :] * forced[rows, lanes].astype(F32)
            argument = current(lanes, d) + spacing_float * (
                sources[d][fine].astype(F32) + drive
            )
            at = lax.rem(place + d, slots) * block
            operand[:, pl.ds(pl.multiple_of(at, block), block)] = argument.astype(BF16)
        held = pl.ds(pl.multiple_of(k * cases, cases), cases)
        half = nodes // 2
        for d in range(slots):
            if d == 2:
                total = jnp.dot(operand[:, :half], a2t[...], preferred_element_type=F32)
                total += jnp.dot(operand[:, half:], a2b[...], preferred_element_type=F32)
            else:
                matrix = {0: a0, 1: a1, 3: a3}[d]
                total = jnp.dot(operand[...], matrix[...], preferred_element_type=F32)
            at = lax.rem(place + d, slots) * block
            mine = operand[:, pl.ds(pl.multiple_of(at, block), block)].astype(F32)
            total += miscs[d][cases : cases + 1, :] * mine
            history[held, d * block : (d + 1) * block] = total

    step(0, lambda lanes, d: miscs[d][:cases, :])

    def later(k, carry):
        before = pl.ds(pl.multiple_of((k - 1) * cases, cases), cases)
        step(k, lambda lanes, d: history[before, lanes])
        return carry

    lax.fori_loop(1, count, later, 0)
    pieces = []
    for g in range(steps):
        at = lax.div(jnp.int32(g), spacing) * cases
        sample = history[pl.ds(pl.multiple_of(at, cases), cases), :]
        high = sample.astype(BF16)
        picked = lax.dot_general(
            high, spread, (((1,), (1,)), ((), ())), preferred_element_type=F32
        )
        if final:
            low = (sample - high.astype(F32)).astype(BF16)
            picked += lax.dot_general(
                low, spread, (((1,), (1,)), ((), ())), preferred_element_type=F32
            )
        pieces.append(picked)
    wave = jnp.transpose(jnp.concatenate(pieces, axis=0))
    if final:
        end = pl.ds(pl.multiple_of((count - 1) * cases, cases), cases)
        for d in range(slots):
            out[d, :cases, :] = history[end, d * block : (d + 1) * block]
            out[d, cases:, :] = wave[d * ports : (d + 1) * ports]
    else:
        for d in range(slots):
            out[d] = wave[d * ports : (d + 1) * ports].astype(BF16)


def sweep(final, meta, matrices, sources, miscs, waves):
    steps, cases, block = sources[0].shape
    ports = waves[0].shape[0]
    rows = cases + ports if final else ports
    nodes = 4 * block
    vmem = pl.BlockSpec(memory_space=pltpu.VMEM)
    return pl.pallas_call(
        functools.partial(sweep_kernel, final),
        out_shape=jax.ShapeDtypeStruct((4, rows, block), F32 if final else BF16),
        in_specs=[pl.BlockSpec(memory_space=pltpu.SMEM)] + [vmem] * 17,
        out_specs=vmem,
        scratch_shapes=[
            pltpu.VMEM((cases, nodes), BF16),
            pltpu.VMEM((steps * cases, nodes), BF16),
            pltpu.VMEM((steps * cases, nodes), F32),
        ],
        cost_estimate=pl.CostEstimate(
            flops=2 * steps * cases * nodes * nodes, bytes_accessed=12 << 20, transcendentals=0
        ),
        compiler_params=pltpu.CompilerParams(vmem_limit_bytes=40 << 20),
        name="sweep_final" if final else "sweep_first",
    )(meta, *matrices, *sources, *miscs, *waves)


def fetch(waves, selector, mesh):
    copies = jnp.broadcast_to(waves, (lax.axis_size("sub"), *waves.shape))
    everyone = lax.all_to_all(copies, "sub", split_axis=0, concat_axis=0, tiled=True)
    return jnp.einsum("jr,rjc->jc", selector, everyone, preferred_element_type=F32).astype(BF16)


def shards(mesh, initial_state, source, inverse_diag, inverse_off, coupling, initial_waves,
           bucket, partner, position_of):
    state, source = initial_state[0], source[0]
    matrix = inverse_off[0]
    steps, cases, block = source.shape
    subs_all = position_of.shape[0]
    ports = coupling.shape[1]
    stride = block // ports
    x = lax.axis_index("blk")
    rel = lax.rem(x + 4 - 2 * lax.rem(lax.axis_index("sub"), 2), 4)

    count = jnp.where(bucket == 0, steps // 4, jnp.where(bucket == 1, steps // 2, steps))
    meta = jnp.concatenate([count, steps // count, x[None]]).astype(jnp.int32)

    half = matrix.shape[0] // 2
    top = move(matrix[:half], mesh, lambda x, r: x - 1 if r == 2 else None)
    bottom = move(matrix[half:], mesh, lambda x, r: x + 1 if r == 2 else None)
    one = move(matrix, mesh, lambda x, r: x - 1 if r == 1 else None)
    three = move(matrix, mesh, lambda x, r: x + 1 if r == 3 else None)
    top = move(top, mesh, lambda x, r: x - 1 if r == 1 else None)
    bottom = move(bottom, mesh, lambda x, r: x + 1 if r == 3 else None)
    matrices = (matrix, one, top, bottom, three)

    injects = jnp.pad(coupling[0][:, None], ((0, 0), (0, stride - 1))).reshape(1, block)
    misc = jnp.concatenate([state, inverse_diag, injects, jnp.zeros((6, block), F32)], axis=0)
    miscs = to_home(misc, mesh)
    sources = to_home(source, mesh)

    identities = jnp.arange(subs_all, dtype=jnp.int32)
    located = jnp.sum(
        jnp.where(partner[0][:, None] == identities[None, :], position_of[None, :], 0), axis=1
    )
    selector = (located[:, None] == identities[None, :]).astype(BF16)

    incoming = fetch(initial_waves[0], selector, mesh)
    slots = sweep(False, meta, matrices, sources, miscs, to_home(incoming, mesh))
    waves = from_home(slots, rel, mesh)
    incoming = fetch(waves, selector, mesh)
    slots = sweep(True, meta, matrices, sources, miscs, to_home(incoming, mesh))
    result = from_home(slots, rel, mesh)
    return result[None, :cases], result[None, cases:]


def solution(mesh):
    return jax.shard_map(
        functools.partial(shards, mesh),
        mesh=mesh,
        in_specs=(
            P("sub", None, "blk"),
            P("sub", None, None, "blk"),
            P("sub", "blk"),
            P("sub", None, "blk"),
            P("sub", "blk"),
            P("sub", "blk", None),
            P("sub"),
            P("sub", "blk"),
            P(),
        ),
        out_specs=(P("sub", None, "blk"), P("sub", "blk", None)),
        check_vma=False,
    )
```

```python
import jax
import jax.numpy as jnp
from jax import lax
from jax.experimental import pallas as pl
from jax.experimental.pallas import tpu as pltpu
from jax.sharding import PartitionSpec as P


F32 = jnp.float32
BF16 = jnp.bfloat16
SLOTS = 4
FAR_ROWS = 1280
WIDE = 5


def hop(array, start, end):
    pairs = []
    for sub in range(32):
        home = 2 * (sub % 2)
        pairs.append((sub * 4 + (home + start) % 4, sub * 4 + (home + end) % 4))
    return lax.ppermute(array, ("sub", "blk"), pairs)


def to_home(array):
    return array, *(hop(array, d, 0) for d in (1, 2, 3))


def turn(array):
    parts = [array]
    for d in (1, 2, 3):
        pairs = [(sub * 4 + (r + d) % 4, sub * 4 + r) for sub in range(32) for r in range(4)]
        parts.append(lax.ppermute(array, ("sub", "blk"), pairs))
    return tuple(parts)


def from_home(slots, rel):
    one, two, three = (hop(slots[d], 0, d) for d in (1, 2, 3))
    return jnp.where(
        rel == 0, slots[0], jnp.where(rel == 1, one, jnp.where(rel == 2, two, three))
    )


def gather_matrix(matrix):
    half = FAR_ROWS
    one, three = hop(matrix, 1, 0), hop(matrix, 3, 0)
    near1, near3 = hop(matrix[:half], 2, 1), hop(matrix[half:], 2, 3)
    upper, lower = hop(near1, 1, 0), hop(near3, 3, 0)
    return matrix, one, upper, lower, three


def port_rows(ports, nodes):
    stride = nodes // ports
    port_at = lax.broadcasted_iota(jnp.int32, (ports, nodes), 0) * stride
    node_at = lax.broadcasted_iota(jnp.int32, (ports, nodes), 1)
    return port_at == node_at


def port_columns(ports, nodes):
    stride = nodes // ports
    port_at = lax.broadcasted_iota(jnp.int32, (nodes, ports), 1) * stride
    node_at = lax.broadcasted_iota(jnp.int32, (nodes, ports), 0)
    return port_at == node_at


def times_matrix(operand, matrices, d):
    if d == 2:
        half = FAR_ROWS
        total = jnp.dot(operand[:, :half], matrices[2][...], preferred_element_type=F32)
        return total + jnp.dot(operand[:, half:], matrices[3][...], preferred_element_type=F32)
    matrix = matrices[{0: 0, 1: 1, 3: 4}[d]]
    return jnp.dot(operand[...], matrix[...], preferred_element_type=F32)


DIAG = 64
INJECT = 65


def sweep_kernel(meta, a0_in, a1_in, a2_in, a3_in, a4_in, s0_in, s1_in, s2_in, s3_in, m0, m1, m2, m3, w0, w1, w2, w3,
                 out, response_out, history_out, operand, state, forced, response, history,
                 sent, a0, a1, a2, a3, a4, s0, s1, s2, s3, arrived):
    steps, cases, block = s0.shape
    ports = w0.shape[0]
    all_ports = SLOTS * ports
    nodes = SLOTS * block
    count, spacing, place = meta[0], meta[1], meta[2]
    spacing_float = spacing.astype(F32)
    matrices, sources, miscs = (a0, a1, a2, a3, a4), (s0, s1, s2, s3), (m0, m1, m2, m3)
    inputs = (s0_in, s1_in, s2_in, s3_in, a0_in, a1_in, a2_in, a3_in, a4_in)
    loads = [
        pltpu.make_async_copy(here, there, arrived.at[i])
        for i, (here, there) in enumerate(zip(inputs, sources + matrices))
    ]
    for load in loads:
        load.start()
    marks = port_rows(all_ports, nodes)
    spread = jnp.where(marks, 1.0, 0.0).astype(BF16)
    waves = jnp.concatenate([w[...] for w in (w0, w1, w2, w3)], axis=0).astype(F32)
    waves = jnp.transpose(waves).astype(BF16)
    forced[...] = jnp.dot(waves, spread, preferred_element_type=F32).astype(BF16)
    state[...] = jnp.where(marks, 1.0, 0.0)

    def argument(current, fine, d):
        rows = pl.ds(pl.multiple_of(fine * cases, cases), cases)
        lanes = slice(d * block, (d + 1) * block)
        drive = miscs[d][INJECT : INJECT + 1, :] * forced[rows, lanes].astype(F32)
        return (current + spacing_float * (sources[d][fine].astype(F32) + drive)).astype(BF16)

    def spot(d):
        return pl.ds(pl.multiple_of(lax.rem(place + d, SLOTS) * block, block), block)

    for load in loads[:SLOTS]:
        load.wait()
    for d in range(SLOTS):
        operand[0, :cases, spot(d)] = argument(miscs[d][:cases, :], spacing - 1, d)
        operand[0, cases:, spot(d)] = spread[:, d * block : (d + 1) * block]

    def send(k):
        rows = pl.ds(pl.multiple_of(k * all_ports, all_ports), all_ports)
        held = pl.ds(pl.multiple_of(k * cases, cases), cases)
        return (
            pltpu.make_async_copy(response.at[rows, :], response_out.at[rows, :], sent.at[0, k]),
            pltpu.make_async_copy(history.at[held, :], history_out.at[held, :], sent.at[1, k]),
        )

    def step(k, carry):
        now, later = lax.rem(k, 2), lax.rem(k + 1, 2)
        fine = jnp.minimum((k + 2) * spacing - 1, steps - 1)
        held = pl.ds(pl.multiple_of(k * cases, cases), cases)
        rows = pl.ds(pl.multiple_of(k * all_ports, all_ports), all_ports)
        for d in range(SLOTS):
            lanes = slice(d * block, (d + 1) * block)
            if carry is None:
                for load in {0: loads[4:5], 1: loads[5:6], 2: loads[6:8], 3: loads[8:]}[d]:
                    load.wait()
            total = times_matrix(operand.at[now], matrices, d)
            diag = miscs[d][DIAG : DIAG + 1, :]
            new = total[:cases] + diag * operand[now, :cases, spot(d)].astype(F32)
            history[held, lanes] = new
            operand[later, :cases, spot(d)] = argument(new, fine, d)
            reply = total[cases:] + diag * state[:, lanes]
            state[:, lanes] = reply
            response[rows, lanes] = reply.astype(BF16)
            operand[later, cases:, spot(d)] = reply.astype(BF16)
        for copy in send(k):
            copy.start()
        return carry

    step(jnp.int32(0), None)
    lax.fori_loop(1, count, step, 0)

    def clear(p, carry):
        rows = pl.ds(pl.multiple_of(p * all_ports, all_ports), all_ports)
        response[rows, :] = jnp.zeros((all_ports, nodes), BF16)
        held = pl.ds(pl.multiple_of(p * cases, cases), cases)
        history[held, :] = jnp.zeros((cases, nodes), F32)
        for copy in send(p):
            copy.start()
        return carry

    lax.fori_loop(count, steps, clear, 0)
    pick = jnp.where(port_columns(all_ports, nodes), 1.0, 0.0).astype(BF16)
    coarse = jnp.dot(history[...].astype(BF16), pick, preferred_element_type=F32)
    forced[: steps * cases, :all_ports] = coarse.astype(BF16)
    pieces = []
    for g in range(steps):
        at = lax.div(jnp.int32(g), spacing) * cases
        rows = pl.ds(pl.multiple_of(at, cases), cases)
        pieces.append(forced[rows, :all_ports].astype(F32))
    wave = jnp.transpose(jnp.concatenate(pieces, axis=0))
    for d in range(SLOTS):
        out[d] = wave[d * ports : (d + 1) * ports].astype(BF16)
    for p in range(steps):
        for copy in send(p):
            copy.wait()


def ports_kernel(meta, response_in, history_in, at_ports, samples, last, response, history,
                 arrived):
    nodes = history.shape[1]
    all_ports = at_ports.shape[1]
    steps = response.shape[0] // all_ports
    cases = history.shape[0] // steps
    first = pltpu.make_async_copy(history_in.at[: steps * cases, :], history, arrived.at[0])
    second = pltpu.make_async_copy(
        response_in.at[: steps * all_ports, :], response, arrived.at[1]
    )
    first.start()
    second.start()
    pick = jnp.where(port_columns(all_ports, nodes), 1.0, 0.0).astype(BF16)
    first.wait()
    high = history[...].astype(BF16)
    low = (history[...] - high.astype(F32)).astype(BF16)
    samples[...] = jnp.dot(high, pick, preferred_element_type=F32)
    samples[...] += jnp.dot(low, pick, preferred_element_type=F32)
    second.wait()
    at_ports[...] = jnp.dot(response[...], pick, preferred_element_type=F32).astype(BF16)
    last[...] = history[pl.ds(pl.multiple_of((meta[0] - 1) * cases, cases), cases), :]


def correct_kernel(meta, response_in, at_ports, last, v0, v1, v2, v3, out, toeplitz,
                   response, arrived):
    cases, nodes = last.shape
    ports, fine_cases = v0.shape
    steps = fine_cases // cases
    block = nodes // SLOTS
    all_ports = SLOTS * ports
    count, spacing = meta[0], meta[1]
    pieces = 4
    part = response.shape[0] // pieces
    copies = []
    for i in range(pieces):
        rows = pl.ds(i * part, part)
        copies.append(
            pltpu.make_async_copy(response_in.at[rows, :], response.at[rows, :], arrived.at[i])
        )
        copies[-1].start()
    drive = jnp.concatenate([v[...] for v in (v0, v1, v2, v3)], axis=0).astype(F32)
    samples_at = jnp.transpose(drive).astype(BF16)
    scratch = toeplitz.at[pl.ds(steps * cases, fine_cases), pl.ds(0, all_ports)]
    scratch[...] = samples_at
    zero = jnp.zeros((cases, all_ports), BF16)
    for i in range(steps):
        fine = jnp.minimum((i + 1) * spacing - 1, steps - 1)
        driven = scratch[pl.ds(pl.multiple_of(fine * cases, cases), cases), :]
        for k in range(i, steps):
            lag = k - i
            toeplitz[k * cases : (k + 1) * cases, lag * all_ports : (lag + 1) * all_ports] = driven
        for lag in range(i + 1, steps):
            toeplitz[i * cases : (i + 1) * cases, lag * all_ports : (lag + 1) * all_ports] = zero
    moved = jnp.dot(toeplitz[: steps * cases, :], at_ports[...], preferred_element_type=F32)
    toe_rows = pl.ds(pl.multiple_of((count - 1) * cases, cases), cases)
    total = last[...]
    for i, copy in enumerate(copies):
        copy.wait()
        rows = slice(i * part, (i + 1) * part)
        total += jnp.dot(toeplitz[toe_rows, rows], response[rows, :], preferred_element_type=F32)
    for d in range(SLOTS):
        out[d, :cases, :] = total[:, d * block : (d + 1) * block]
    return moved


def correct_whole(meta, response, at_ports, samples, last, v0, v1, v2, v3, out, toeplitz, held,
                  response_in, arrived):
    cases = last.shape[0]
    ports, fine_cases = v0.shape
    held[...] = samples[...] + correct_kernel(
        meta, response, at_ports, last, v0, v1, v2, v3, out, toeplitz, response_in, arrived
    )
    pieces = []
    for g in range(fine_cases // cases):
        at = lax.div(jnp.int32(g), meta[1]) * cases
        pieces.append(held[pl.ds(pl.multiple_of(at, cases), cases), :])
    wave = jnp.transpose(jnp.concatenate(pieces, axis=0))
    for d in range(SLOTS):
        out[d, cases:, :] = wave[d * ports : (d + 1) * ports]


def call(kernel, outs, scratch, flops, limit, meta, *operands, hbm_outs=(), hbm_ins=()):
    vmem, hbm = pl.BlockSpec(memory_space=pltpu.VMEM), pl.BlockSpec(memory_space=pltpu.HBM)
    outs = tuple(outs)
    return pl.pallas_call(
        kernel,
        out_shape=outs,
        in_specs=[pl.BlockSpec(memory_space=pltpu.SMEM)]
        + [hbm if i in hbm_ins else vmem for i in range(len(operands))],
        out_specs=tuple(hbm if i in hbm_outs else vmem for i in range(len(outs))),
        scratch_shapes=scratch,
        cost_estimate=pl.CostEstimate(flops=flops, bytes_accessed=12 << 20, transcendentals=0),
        compiler_params=pltpu.CompilerParams(vmem_limit_bytes=limit << 20),
    )(meta, *operands)


def fetch(waves, selector):
    copies = jnp.broadcast_to(waves, (lax.axis_size("sub"), *waves.shape))
    everyone = lax.all_to_all(copies, "sub", split_axis=0, concat_axis=0, tiled=True)
    return jnp.einsum("jr,rjc->jc", selector, everyone, preferred_element_type=F32)


def shards(initial_state, source, inverse_diag, inverse_off, coupling, initial_waves,
           bucket, partner, position_of):
    state, source, matrix = initial_state[0], source[0], inverse_off[0]
    steps, cases, block = source.shape
    nodes = matrix.shape[0]
    subs_all = position_of.shape[0]
    ports = coupling.shape[1]
    all_ports = SLOTS * ports
    x = lax.axis_index("blk")
    rel = lax.rem(x + 4 - 2 * lax.rem(lax.axis_index("sub"), 2), 4)

    count = jnp.where(bucket == 0, steps // 4, jnp.where(bucket == 1, steps // 2, steps))
    spacing = steps // count
    meta = jnp.concatenate([count, spacing, x[None]]).astype(jnp.int32)

    matrices = gather_matrix(matrix)
    injects = jnp.pad(coupling[0][:, None], ((0, 0), (0, block // ports - 1))).reshape(1, block)
    misc = jnp.concatenate([state, inverse_diag, injects, jnp.zeros((6, block), F32)], axis=0)
    miscs = to_home(misc)
    sources = to_home(source)

    identities = jnp.arange(subs_all, dtype=jnp.int32)
    located = jnp.sum(
        jnp.where(partner[0][:, None] == identities[None, :], position_of[None, :], 0), axis=1
    )
    selector = (located[:, None] == identities[None, :]).astype(BF16)

    before = fetch(initial_waves[0], selector)
    incoming = to_home(before.astype(BF16))

    shape = jax.ShapeDtypeStruct
    slots, response, history = call(
        sweep_kernel,
        (shape((SLOTS, ports, steps * cases), BF16), shape((WIDE * steps * all_ports, nodes), BF16),
         shape((WIDE * steps * cases, nodes), F32)),
        [pltpu.VMEM((2, cases + all_ports, nodes), BF16), pltpu.VMEM((all_ports, nodes), F32),
         pltpu.VMEM((steps * cases, nodes), BF16), pltpu.VMEM((steps * all_ports, nodes), BF16),
         pltpu.VMEM((steps * cases, nodes), F32), pltpu.SemaphoreType.DMA((2, steps)),
         *(pltpu.VMEM(m.shape, BF16) for m in matrices), *(pltpu.VMEM(a.shape, BF16) for a in sources),
         pltpu.SemaphoreType.DMA((9,))],
        2 * steps * (cases + all_ports) * nodes * nodes, LIMITS[0], meta,
        *matrices, *sources, *miscs, *incoming, hbm_outs=(1, 2), hbm_ins=range(9),
    )
    at_ports, samples, last = call(
        ports_kernel,
        (shape((steps * all_ports, all_ports), BF16), shape((steps * cases, all_ports), F32),
         shape((cases, nodes), F32)),
        [pltpu.VMEM((steps * all_ports, nodes), BF16), pltpu.VMEM((steps * cases, nodes), F32),
         pltpu.SemaphoreType.DMA((2,))],
        2 * steps * (all_ports + 2 * cases) * nodes * all_ports, LIMITS[1], meta,
        response, history, hbm_ins=(0, 1),
    )

    waves = from_home(slots, rel)
    after = fetch(waves, selector)
    gain = spacing.astype(F32) * coupling[0]
    drives = turn((gain[:, None] * (after - before)).astype(BF16))
    (result,) = call(
        correct_whole,
        (shape((SLOTS, cases + ports, block), F32),),
        [pltpu.VMEM((2 * steps * cases, steps * all_ports), BF16),
         pltpu.VMEM((steps * cases, all_ports), F32),
         pltpu.VMEM((steps * all_ports, nodes), BF16), pltpu.SemaphoreType.DMA((4,))],
        2 * cases * steps * all_ports * nodes, LIMITS[2], meta,
        response, at_ports, samples, last, *drives, hbm_ins=(0,),
    )
    result = from_home(result, rel)
    return result[None, :cases], result[None, cases:]


LIMITS = (45, 45, 45)


def solution(mesh):
    return jax.shard_map(
        shards,
        mesh=mesh,
        in_specs=(
            P("sub", None, "blk"),
            P("sub", None, None, "blk"),
            P("sub", "blk"),
            P("sub", None, "blk"),
            P("sub", "blk"),
            P("sub", "blk", None),
            P("sub"),
            P("sub", "blk"),
            P(),
        ),
        out_specs=(P("sub", None, "blk"), P("sub", "blk", None)),
        check_vma=False,
    )
```

```python
import jax
import jax.numpy as jnp
from jax import lax
from jax.experimental import pallas as pl
from jax.experimental.pallas import tpu as pltpu
from jax.sharding import PartitionSpec as P


F32 = jnp.float32
BF16 = jnp.bfloat16
SLOTS = 4
FAR_ROWS = 1280
WIDE = 5


def hop(array, start, end):
    pairs = []
    for sub in range(32):
        home = 2 * (sub % 2)
        pairs.append((sub * 4 + (home + start) % 4, sub * 4 + (home + end) % 4))
    return lax.ppermute(array, ("sub", "blk"), pairs)


def to_home(array):
    return array, *(hop(array, d, 0) for d in (1, 2, 3))


def turn(array):
    parts = [array]
    for d in (1, 2, 3):
        pairs = [(sub * 4 + (r + d) % 4, sub * 4 + r) for sub in range(32) for r in range(4)]
        parts.append(lax.ppermute(array, ("sub", "blk"), pairs))
    return tuple(parts)


def from_home(slots):
    return slots[0], *(hop(slots[d], 0, d) for d in (1, 2, 3))


def mine(parts, rel, rows=slice(None)):
    zero, one, two, three = (part[rows] for part in parts)
    return jnp.where(rel == 0, zero, jnp.where(rel == 1, one, jnp.where(rel == 2, two, three)))


def gather_matrix(matrix):
    half = FAR_ROWS
    one, three = hop(matrix, 1, 0), hop(matrix, 3, 0)
    near1, near3 = hop(matrix[:half], 2, 1), hop(matrix[half:], 2, 3)
    upper, lower = hop(near1, 1, 0), hop(near3, 3, 0)
    return matrix, one, upper, lower, three


def port_rows(ports, nodes):
    stride = nodes // ports
    port_at = lax.broadcasted_iota(jnp.int32, (ports, nodes), 0) * stride
    node_at = lax.broadcasted_iota(jnp.int32, (ports, nodes), 1)
    return port_at == node_at


def port_columns(ports, nodes):
    stride = nodes // ports
    port_at = lax.broadcasted_iota(jnp.int32, (nodes, ports), 1) * stride
    node_at = lax.broadcasted_iota(jnp.int32, (nodes, ports), 0)
    return port_at == node_at


def times_matrix(operand, matrices, d):
    if d == 2:
        half = FAR_ROWS
        total = jnp.dot(operand[:, :half], matrices[2][...], preferred_element_type=F32)
        return total + jnp.dot(operand[:, half:], matrices[3][...], preferred_element_type=F32)
    matrix = matrices[{0: 0, 1: 1, 3: 4}[d]]
    return jnp.dot(operand[...], matrix[...], preferred_element_type=F32)


DIAG = 64
INJECT = 65


def sweep_kernel(meta, a0_in, a1_in, a2_in, a3_in, a4_in, s0_in, s1_in, s2_in, s3_in, m0, m1, m2, m3, w0, w1, w2, w3,
                 out, response_out, history_out, operand, state, forced, response, history,
                 sent, a0, a1, a2, a3, a4, s0, s1, s2, s3, arrived):
    steps, cases, block = s0.shape
    ports = w0.shape[0]
    all_ports = SLOTS * ports
    nodes = SLOTS * block
    count, spacing, place = meta[0], meta[1], meta[2]
    spacing_float = spacing.astype(F32)
    matrices, sources, miscs = (a0, a1, a2, a3, a4), (s0, s1, s2, s3), (m0, m1, m2, m3)
    inputs = (s0_in, s1_in, s2_in, s3_in, a0_in, a1_in, a2_in, a3_in, a4_in)
    loads = [
        pltpu.make_async_copy(here, there, arrived.at[i])
        for i, (here, there) in enumerate(zip(inputs, sources + matrices))
    ]
    for load in loads:
        load.start()
    marks = port_rows(all_ports, nodes)
    spread = jnp.where(marks, 1.0, 0.0).astype(BF16)
    waves = jnp.concatenate([w[...] for w in (w0, w1, w2, w3)], axis=0).astype(F32)
    waves = jnp.transpose(waves).astype(BF16)
    forced[...] = jnp.dot(waves, spread, preferred_element_type=F32).astype(BF16)
    state[...] = jnp.where(marks, 1.0, 0.0)

    def argument(current, fine, d):
        rows = pl.ds(pl.multiple_of(fine * cases, cases), cases)
        lanes = slice(d * block, (d + 1) * block)
        drive = miscs[d][INJECT : INJECT + 1, :] * forced[rows, lanes].astype(F32)
        return (current + spacing_float * (sources[d][fine].astype(F32) + drive)).astype(BF16)

    def spot(d):
        return pl.ds(pl.multiple_of(lax.rem(place + d, SLOTS) * block, block), block)

    for load in loads[:SLOTS]:
        load.wait()
    for d in range(SLOTS):
        operand[0, :cases, spot(d)] = argument(miscs[d][:cases, :], spacing - 1, d)
        operand[0, cases:, spot(d)] = spread[:, d * block : (d + 1) * block]

    def send(k):
        rows = pl.ds(pl.multiple_of(k * all_ports, all_ports), all_ports)
        held = pl.ds(pl.multiple_of(k * cases, cases), cases)
        return (
            pltpu.make_async_copy(response.at[rows, :], response_out.at[rows, :], sent.at[0, k]),
            pltpu.make_async_copy(history.at[held, :], history_out.at[held, :], sent.at[1, k]),
        )

    def step(k, carry):
        now, later = lax.rem(k, 2), lax.rem(k + 1, 2)
        fine = jnp.minimum((k + 2) * spacing - 1, steps - 1)
        held = pl.ds(pl.multiple_of(k * cases, cases), cases)
        rows = pl.ds(pl.multiple_of(k * all_ports, all_ports), all_ports)
        for d in range(SLOTS):
            lanes = slice(d * block, (d + 1) * block)
            if carry is None:
                for load in {0: loads[4:5], 1: loads[5:6], 2: loads[6:8], 3: loads[8:]}[d]:
                    load.wait()
            total = times_matrix(operand.at[now], matrices, d)
            diag = miscs[d][DIAG : DIAG + 1, :]
            new = total[:cases] + diag * operand[now, :cases, spot(d)].astype(F32)
            history[held, lanes] = new
            operand[later, :cases, spot(d)] = argument(new, fine, d)
            reply = total[cases:] + diag * state[:, lanes]
            state[:, lanes] = reply
            response[rows, lanes] = reply.astype(BF16)
            operand[later, cases:, spot(d)] = reply.astype(BF16)
        for copy in send(k):
            copy.start()
        return carry

    step(jnp.int32(0), None)
    lax.fori_loop(1, count, step, 0)

    def clear(p, carry):
        rows = pl.ds(pl.multiple_of(p * all_ports, all_ports), all_ports)
        response[rows, :] = jnp.zeros((all_ports, nodes), BF16)
        held = pl.ds(pl.multiple_of(p * cases, cases), cases)
        history[held, :] = jnp.zeros((cases, nodes), F32)
        for copy in send(p):
            copy.start()
        return carry

    lax.fori_loop(count, steps, clear, 0)
    pick = jnp.where(port_columns(all_ports, nodes), 1.0, 0.0).astype(BF16)
    coarse = jnp.dot(history[...].astype(BF16), pick, preferred_element_type=F32)
    forced[: steps * cases, :all_ports] = coarse.astype(BF16)
    pieces = []
    for g in range(steps):
        at = lax.div(jnp.int32(g), spacing) * cases
        rows = pl.ds(pl.multiple_of(at, cases), cases)
        pieces.append(forced[rows, :all_ports].astype(F32))
    wave = jnp.transpose(jnp.concatenate(pieces, axis=0))
    for d in range(SLOTS):
        out[d] = wave[d * ports : (d + 1) * ports].astype(BF16)
    for p in range(steps):
        for copy in send(p):
            copy.wait()


def ports_kernel(meta, response_in, history_in, at_ports, samples, last, response, history,
                 arrived):
    nodes = history.shape[1]
    all_ports = at_ports.shape[1]
    steps = response.shape[0] // all_ports
    cases = history.shape[0] // steps
    first = pltpu.make_async_copy(history_in.at[: steps * cases, :], history, arrived.at[0])
    second = pltpu.make_async_copy(
        response_in.at[: steps * all_ports, :], response, arrived.at[1]
    )
    first.start()
    second.start()
    pick = jnp.where(port_columns(all_ports, nodes), 1.0, 0.0).astype(BF16)
    first.wait()
    high = history[...].astype(BF16)
    low = (history[...] - high.astype(F32)).astype(BF16)
    samples[...] = jnp.dot(high, pick, preferred_element_type=F32)
    samples[...] += jnp.dot(low, pick, preferred_element_type=F32)
    second.wait()
    at_ports[...] = jnp.dot(response[...], pick, preferred_element_type=F32).astype(BF16)
    last[...] = history[pl.ds(pl.multiple_of((meta[0] - 1) * cases, cases), cases), :]


def correct_kernel(meta, response_in, at_ports, last, v0, v1, v2, v3, out, toeplitz,
                   response, arrived):
    cases, nodes = last.shape
    ports, fine_cases = v0.shape
    steps = fine_cases // cases
    block = nodes // SLOTS
    all_ports = SLOTS * ports
    count, spacing = meta[0], meta[1]
    pieces = 4
    part = response.shape[0] // pieces
    copies = []
    for i in range(pieces):
        rows = pl.ds(i * part, part)
        copies.append(
            pltpu.make_async_copy(response_in.at[rows, :], response.at[rows, :], arrived.at[i])
        )
        copies[-1].start()
    drive = jnp.concatenate([v[...] for v in (v0, v1, v2, v3)], axis=0).astype(F32)
    samples_at = jnp.transpose(drive).astype(BF16)
    scratch = toeplitz.at[pl.ds(steps * cases, fine_cases), pl.ds(0, all_ports)]
    scratch[...] = samples_at
    zero = jnp.zeros((cases, all_ports), BF16)
    for i in range(steps):
        fine = jnp.minimum((i + 1) * spacing - 1, steps - 1)
        driven = scratch[pl.ds(pl.multiple_of(fine * cases, cases), cases), :]
        for k in range(i, steps):
            lag = k - i
            toeplitz[k * cases : (k + 1) * cases, lag * all_ports : (lag + 1) * all_ports] = driven
        for lag in range(i + 1, steps):
            toeplitz[i * cases : (i + 1) * cases, lag * all_ports : (lag + 1) * all_ports] = zero
    moved = jnp.dot(toeplitz[: steps * cases, :], at_ports[...], preferred_element_type=F32)
    toe_rows = pl.ds(pl.multiple_of((count - 1) * cases, cases), cases)
    total = last[...]
    for i, copy in enumerate(copies):
        copy.wait()
        rows = slice(i * part, (i + 1) * part)
        total += jnp.dot(toeplitz[toe_rows, rows], response[rows, :], preferred_element_type=F32)
    for d in range(SLOTS):
        out[d, :cases, :] = total[:, d * block : (d + 1) * block]
    return moved


def correct_whole(meta, response, at_ports, samples, last, v0, v1, v2, v3, out, toeplitz, held,
                  response_in, arrived):
    cases = last.shape[0]
    ports, fine_cases = v0.shape
    held[...] = samples[...] + correct_kernel(
        meta, response, at_ports, last, v0, v1, v2, v3, out, toeplitz, response_in, arrived
    )
    pieces = []
    for g in range(fine_cases // cases):
        at = lax.div(jnp.int32(g), meta[1]) * cases
        pieces.append(held[pl.ds(pl.multiple_of(at, cases), cases), :])
    wave = jnp.transpose(jnp.concatenate(pieces, axis=0))
    for d in range(SLOTS):
        out[d, cases:, :] = wave[d * ports : (d + 1) * ports]


def call(kernel, outs, scratch, flops, limit, meta, *operands, hbm_outs=(), hbm_ins=()):
    vmem, hbm = pl.BlockSpec(memory_space=pltpu.VMEM), pl.BlockSpec(memory_space=pltpu.HBM)
    outs = tuple(outs)
    return pl.pallas_call(
        kernel,
        out_shape=outs,
        in_specs=[pl.BlockSpec(memory_space=pltpu.SMEM)]
        + [hbm if i in hbm_ins else vmem for i in range(len(operands))],
        out_specs=tuple(hbm if i in hbm_outs else vmem for i in range(len(outs))),
        scratch_shapes=scratch,
        cost_estimate=pl.CostEstimate(flops=flops, bytes_accessed=12 << 20, transcendentals=0),
        compiler_params=pltpu.CompilerParams(vmem_limit_bytes=limit << 20),
    )(meta, *operands)


def first_fetch(waves, partner, position_of):
    subs = lax.axis_size("sub")
    ports = waves.shape[0]
    ids = jnp.pad(partner.astype(BF16)[None, :], ((0, 15), (0, waves.shape[1] - ports)))
    copies = jnp.broadcast_to(jnp.concatenate([waves, ids], axis=0), (subs, ports + 16, waves.shape[1]))
    everyone = lax.all_to_all(copies, "sub", split_axis=0, concat_axis=0, tiled=True)
    identities = jnp.arange(subs, dtype=jnp.int32)

    def locate(ids):
        return jnp.sum(
            jnp.where(ids[..., None] == identities, position_of, 0), axis=-1, dtype=jnp.int32
        )

    selector = (locate(partner)[:, None] == identities[None, :]).astype(BF16)
    incoming = jnp.einsum(
        "jr,rjc->jc", selector, everyone[:, :ports], preferred_element_type=F32
    )
    return incoming, locate(everyone[:, ports, :ports].astype(jnp.int32))


def second_fetch(waves, located):
    subs = lax.axis_size("sub")
    sub = lax.axis_index("sub")
    swap = [(s * SLOTS + r, (s ^ 1) * SLOTS + r) for s in range(subs) for r in range(SLOTS)]
    others = lax.ppermute(waves, ("sub", "blk"), swap)
    pairs = located.reshape(subs // 2, 2, -1)
    wanted = jnp.where(lax.rem(sub, 2) == 0, pairs[:, 0], pairs[:, 1])[:, :, None]
    zero = jnp.zeros((), BF16)
    sent = jnp.where(
        wanted == sub, waves[None], jnp.where(wanted == (sub ^ 1), others[None], zero)
    )
    groups = [[s for s in range(subs) if s % 2 == core] for core in (0, 1)]
    parts = lax.all_to_all(
        sent, "sub", split_axis=0, concat_axis=0, axis_index_groups=groups, tiled=True
    )
    return jnp.sum(parts.astype(F32), axis=0)


def shards(initial_state, source, inverse_diag, inverse_off, coupling, initial_waves,
           bucket, partner, position_of):
    state, source, matrix = initial_state[0], source[0], inverse_off[0]
    steps, cases, block = source.shape
    nodes = matrix.shape[0]
    ports = coupling.shape[1]
    all_ports = SLOTS * ports
    x = lax.axis_index("blk")
    rel = lax.rem(x + 4 - 2 * lax.rem(lax.axis_index("sub"), 2), 4)

    count = jnp.where(bucket == 0, steps // 4, jnp.where(bucket == 1, steps // 2, steps))
    spacing = steps // count
    meta = jnp.concatenate([count, spacing, x[None]]).astype(jnp.int32)

    matrices = gather_matrix(matrix)
    injects = jnp.pad(coupling[0][:, None], ((0, 0), (0, block // ports - 1))).reshape(1, block)
    misc = jnp.concatenate([state, inverse_diag, injects, jnp.zeros((6, block), F32)], axis=0)
    miscs = to_home(misc)
    sources = to_home(source)

    before, located = first_fetch(initial_waves[0], partner[0], position_of)
    incoming = to_home(before.astype(BF16))

    shape = jax.ShapeDtypeStruct
    slots, response, history = call(
        sweep_kernel,
        (shape((SLOTS, ports, steps * cases), BF16), shape((WIDE * steps * all_ports, nodes), BF16),
         shape((WIDE * steps * cases, nodes), F32)),
        [pltpu.VMEM((2, cases + all_ports, nodes), BF16), pltpu.VMEM((all_ports, nodes), F32),
         pltpu.VMEM((steps * cases, nodes), BF16), pltpu.VMEM((steps * all_ports, nodes), BF16),
         pltpu.VMEM((steps * cases, nodes), F32), pltpu.SemaphoreType.DMA((2, steps)),
         *(pltpu.VMEM(m.shape, BF16) for m in matrices), *(pltpu.VMEM(a.shape, BF16) for a in sources),
         pltpu.SemaphoreType.DMA((9,))],
        2 * steps * (cases + all_ports) * nodes * nodes, LIMITS[0], meta,
        *matrices, *sources, *miscs, *incoming, hbm_outs=(1, 2), hbm_ins=range(9),
    )
    at_ports, samples, last = call(
        ports_kernel,
        (shape((steps * all_ports, all_ports), BF16), shape((steps * cases, all_ports), F32),
         shape((cases, nodes), F32)),
        [pltpu.VMEM((steps * all_ports, nodes), BF16), pltpu.VMEM((steps * cases, nodes), F32),
         pltpu.SemaphoreType.DMA((2,))],
        2 * steps * (all_ports + 2 * cases) * nodes * all_ports, LIMITS[1], meta,
        response, history, hbm_ins=(0, 1),
    )

    waves = mine(from_home(slots), rel)
    after = second_fetch(waves, located)
    gain = spacing.astype(F32) * coupling[0]
    drives = turn((gain[:, None] * (after - before)).astype(BF16))
    (result,) = call(
        correct_whole,
        (shape((SLOTS, cases + ports, block), F32),),
        [pltpu.VMEM((2 * steps * cases, steps * all_ports), BF16),
         pltpu.VMEM((steps * cases, all_ports), F32),
         pltpu.VMEM((steps * all_ports, nodes), BF16), pltpu.SemaphoreType.DMA((4,))],
        2 * cases * steps * all_ports * nodes, LIMITS[2], meta,
        response, at_ports, samples, last, *drives, hbm_ins=(0,),
    )
    parts = from_home(result)
    last = mine(parts, rel, slice(0, cases))
    waveform = mine(parts, rel, slice(cases, None))
    return last[None], waveform[None]


LIMITS = (45, 45, 45)


def solution(mesh):
    return jax.shard_map(
        shards,
        mesh=mesh,
        in_specs=(
            P("sub", None, "blk"),
            P("sub", None, None, "blk"),
            P("sub", "blk"),
            P("sub", None, "blk"),
            P("sub", "blk"),
            P("sub", "blk", None),
            P("sub"),
            P("sub", "blk"),
            P(),
        ),
        out_specs=(P("sub", None, "blk"), P("sub", "blk", None)),
        check_vma=False,
    )
```

```python
import jax
import jax.numpy as jnp
from jax import lax
from jax.experimental import pallas as pl
from jax.experimental.pallas import tpu as pltpu
from jax.sharding import PartitionSpec as P


F32 = jnp.float32
BF16 = jnp.bfloat16
SLOTS = 4
FAR_ROWS = 1280
WIDE = 5


def hop(array, start, end):
    pairs = []
    for sub in range(32):
        home = 2 * (sub % 2)
        pairs.append((sub * 4 + (home + start) % 4, sub * 4 + (home + end) % 4))
    return lax.ppermute(array, ("sub", "blk"), pairs)


def to_home(array):
    return array, *(hop(array, d, 0) for d in (1, 2, 3))


def turn(array):
    parts = [array]
    for d in (1, 2, 3):
        pairs = [(sub * 4 + (r + d) % 4, sub * 4 + r) for sub in range(32) for r in range(4)]
        parts.append(lax.ppermute(array, ("sub", "blk"), pairs))
    return tuple(parts)


def from_home(slots):
    return slots[0], *(hop(slots[d], 0, d) for d in (1, 2, 3))


def mine(parts, rel, rows=slice(None)):
    zero, one, two, three = (part[rows] for part in parts)
    return jnp.where(rel == 0, zero, jnp.where(rel == 1, one, jnp.where(rel == 2, two, three)))


def gather_matrix(matrix):
    half = FAR_ROWS
    one, three = hop(matrix, 1, 0), hop(matrix, 3, 0)
    near1, near3 = hop(matrix[:half], 2, 1), hop(matrix[half:], 2, 3)
    upper, lower = hop(near1, 1, 0), hop(near3, 3, 0)
    return matrix, one, upper, lower, three


def port_rows(ports, nodes):
    stride = nodes // ports
    port_at = lax.broadcasted_iota(jnp.int32, (ports, nodes), 0) * stride
    node_at = lax.broadcasted_iota(jnp.int32, (ports, nodes), 1)
    return port_at == node_at


def port_columns(ports, nodes):
    stride = nodes // ports
    port_at = lax.broadcasted_iota(jnp.int32, (nodes, ports), 1) * stride
    node_at = lax.broadcasted_iota(jnp.int32, (nodes, ports), 0)
    return port_at == node_at


def times_matrix(operand, matrices, d):
    if d == 2:
        half = FAR_ROWS
        total = jnp.dot(operand[:, :half], matrices[2][...], preferred_element_type=F32)
        return total + jnp.dot(operand[:, half:], matrices[3][...], preferred_element_type=F32)
    matrix = matrices[{0: 0, 1: 1, 3: 4}[d]]
    return jnp.dot(operand[...], matrix[...], preferred_element_type=F32)


DIAG = 0
INJECT = 1


def sweep_kernel(meta, a0_in, a1_in, a2_in, a3_in, a4_in, s0_in, s1_in, s2_in, s3_in, m0, m1, m2, m3, w0, w1, w2, w3,
                 out, response_out, history_out, operand, state, forced, response, history,
                 sent, a0, a1, a2, a3, a4, s0, s1, s2, s3, arrived):
    later_steps, cases, block = s0.shape
    steps = later_steps + 1
    ports = w0.shape[0] - cases
    all_ports = SLOTS * ports
    nodes = SLOTS * block
    count, spacing, place = meta[0], meta[1], meta[2]
    spacing_float = spacing.astype(F32)
    matrices, sources, miscs = (a0, a1, a2, a3, a4), (s0, s1, s2, s3), (m0, m1, m2, m3)
    inputs = (s0_in, s1_in, s2_in, s3_in, a0_in, a1_in, a2_in, a3_in, a4_in)
    loads = [
        pltpu.make_async_copy(here, there, arrived.at[i])
        for i, (here, there) in enumerate(zip(inputs, sources + matrices))
    ]
    for load in loads:
        load.start()
    marks = port_rows(all_ports, nodes)
    spread = jnp.where(marks, 1.0, 0.0).astype(BF16)
    waves = jnp.concatenate([w[:ports, :] for w in (w0, w1, w2, w3)], axis=0).astype(F32)
    waves = jnp.transpose(waves).astype(BF16)
    forced[...] = jnp.dot(waves, spread, preferred_element_type=F32).astype(BF16)
    state[...] = jnp.where(marks, 1.0, 0.0)

    def argument(current, fine, d):
        rows = pl.ds(pl.multiple_of(fine * cases, cases), cases)
        lanes = slice(d * block, (d + 1) * block)
        drive = miscs[d][INJECT : INJECT + 1, :] * forced[rows, lanes].astype(F32)
        return (current + spacing_float * (sources[d][fine - 1].astype(F32) + drive)).astype(BF16)

    def spot(d):
        return pl.ds(pl.multiple_of(lax.rem(place + d, SLOTS) * block, block), block)

    for d, late in enumerate((w0, w1, w2, w3)):
        operand[0, :cases, spot(d)] = late[ports:, :]
        operand[0, cases:, spot(d)] = spread[:, d * block : (d + 1) * block]

    def send(k):
        rows = pl.ds(pl.multiple_of(k * all_ports, all_ports), all_ports)
        held = pl.ds(pl.multiple_of(k * cases, cases), cases)
        return (
            pltpu.make_async_copy(response.at[rows, :], response_out.at[rows, :], sent.at[0, k]),
            pltpu.make_async_copy(history.at[held, :], history_out.at[held, :], sent.at[1, k]),
        )

    def step(k, carry):
        now, later = lax.rem(k, 2), lax.rem(k + 1, 2)
        fine = jnp.minimum((k + 2) * spacing - 1, steps - 1)
        held = pl.ds(pl.multiple_of(k * cases, cases), cases)
        rows = pl.ds(pl.multiple_of(k * all_ports, all_ports), all_ports)
        for d in range(SLOTS):
            lanes = slice(d * block, (d + 1) * block)
            if carry is None:
                for load in {0: loads[4:5], 1: loads[5:6], 2: loads[6:8], 3: loads[8:]}[d]:
                    load.wait()
            total = times_matrix(operand.at[now], matrices, d)
            diag = miscs[d][DIAG : DIAG + 1, :]
            new = total[:cases] + diag * operand[now, :cases, spot(d)].astype(F32)
            history[held, lanes] = new
            operand[later, :cases, spot(d)] = argument(new, fine, d)
            reply = total[cases:] + diag * state[:, lanes]
            state[:, lanes] = reply
            response[rows, lanes] = reply.astype(BF16)
            operand[later, cases:, spot(d)] = reply.astype(BF16)
        for copy in send(k):
            copy.start()
        return carry

    for load in loads[:SLOTS]:
        load.wait()
    step(jnp.int32(0), None)
    lax.fori_loop(1, count, step, 0)

    def clear(p, carry):
        rows = pl.ds(pl.multiple_of(p * all_ports, all_ports), all_ports)
        response[rows, :] = jnp.zeros((all_ports, nodes), BF16)
        held = pl.ds(pl.multiple_of(p * cases, cases), cases)
        history[held, :] = jnp.zeros((cases, nodes), F32)
        for copy in send(p):
            copy.start()
        return carry

    lax.fori_loop(count, steps, clear, 0)
    pick = jnp.where(port_columns(all_ports, nodes), 1.0, 0.0).astype(BF16)
    coarse = jnp.dot(history[...].astype(BF16), pick, preferred_element_type=F32)
    forced[: steps * cases, :all_ports] = coarse.astype(BF16)
    pieces = []
    for g in range(steps):
        at = lax.div(jnp.int32(g), spacing) * cases
        rows = pl.ds(pl.multiple_of(at, cases), cases)
        pieces.append(forced[rows, :all_ports].astype(F32))
    wave = jnp.transpose(jnp.concatenate(pieces, axis=0))
    for d in range(SLOTS):
        out[d] = wave[d * ports : (d + 1) * ports].astype(BF16)
    for p in range(steps):
        for copy in send(p):
            copy.wait()


def ports_kernel(meta, response_in, history_in, at_ports, samples, last, response, history,
                 arrived):
    nodes = history.shape[1]
    all_ports = at_ports.shape[1]
    steps = response.shape[0] // all_ports
    cases = history.shape[0] // steps
    first = pltpu.make_async_copy(history_in.at[: steps * cases, :], history, arrived.at[0])
    second = pltpu.make_async_copy(
        response_in.at[: steps * all_ports, :], response, arrived.at[1]
    )
    first.start()
    second.start()
    pick = jnp.where(port_columns(all_ports, nodes), 1.0, 0.0).astype(BF16)
    first.wait()
    high = history[...].astype(BF16)
    low = (history[...] - high.astype(F32)).astype(BF16)
    samples[...] = jnp.dot(high, pick, preferred_element_type=F32)
    samples[...] += jnp.dot(low, pick, preferred_element_type=F32)
    second.wait()
    at_ports[...] = jnp.dot(response[...], pick, preferred_element_type=F32).astype(BF16)
    last[...] = history[pl.ds(pl.multiple_of((meta[0] - 1) * cases, cases), cases), :]


def correct_kernel(meta, response_in, at_ports, last, v0, v1, v2, v3, out, toeplitz,
                   response, arrived):
    cases, nodes = last.shape
    ports, fine_cases = v0.shape
    steps = fine_cases // cases
    block = nodes // SLOTS
    all_ports = SLOTS * ports
    count, spacing = meta[0], meta[1]
    pieces = 4
    part = response.shape[0] // pieces
    copies = []
    for i in range(pieces):
        rows = pl.ds(i * part, part)
        copies.append(
            pltpu.make_async_copy(response_in.at[rows, :], response.at[rows, :], arrived.at[i])
        )
        copies[-1].start()
    drive = jnp.concatenate([v[...] for v in (v0, v1, v2, v3)], axis=0).astype(F32)
    samples_at = jnp.transpose(drive).astype(BF16)
    scratch = toeplitz.at[pl.ds(steps * cases, fine_cases), pl.ds(0, all_ports)]
    scratch[...] = samples_at
    zero = jnp.zeros((cases, all_ports), BF16)
    for i in range(steps):
        fine = jnp.minimum((i + 1) * spacing - 1, steps - 1)
        driven = scratch[pl.ds(pl.multiple_of(fine * cases, cases), cases), :]
        for k in range(i, steps):
            lag = k - i
            toeplitz[k * cases : (k + 1) * cases, lag * all_ports : (lag + 1) * all_ports] = driven
        for lag in range(i + 1, steps):
            toeplitz[i * cases : (i + 1) * cases, lag * all_ports : (lag + 1) * all_ports] = zero
    moved = jnp.dot(toeplitz[: steps * cases, :], at_ports[...], preferred_element_type=F32)
    toe_rows = pl.ds(pl.multiple_of((count - 1) * cases, cases), cases)
    total = last[...]
    for i, copy in enumerate(copies):
        copy.wait()
        rows = slice(i * part, (i + 1) * part)
        total += jnp.dot(toeplitz[toe_rows, rows], response[rows, :], preferred_element_type=F32)
    for d in range(SLOTS):
        out[d, :cases, :] = total[:, d * block : (d + 1) * block]
    return moved


def correct_whole(meta, response, at_ports, samples, last, v0, v1, v2, v3, out, toeplitz, held,
                  response_in, arrived):
    cases = last.shape[0]
    ports, fine_cases = v0.shape
    held[...] = samples[...] + correct_kernel(
        meta, response, at_ports, last, v0, v1, v2, v3, out, toeplitz, response_in, arrived
    )
    pieces = []
    for g in range(fine_cases // cases):
        at = lax.div(jnp.int32(g), meta[1]) * cases
        pieces.append(held[pl.ds(pl.multiple_of(at, cases), cases), :])
    wave = jnp.transpose(jnp.concatenate(pieces, axis=0))
    for d in range(SLOTS):
        out[d, cases:, :] = wave[d * ports : (d + 1) * ports]


def call(kernel, outs, scratch, flops, limit, meta, *operands, hbm_outs=(), hbm_ins=()):
    vmem, hbm = pl.BlockSpec(memory_space=pltpu.VMEM), pl.BlockSpec(memory_space=pltpu.HBM)
    outs = tuple(outs)
    return pl.pallas_call(
        kernel,
        out_shape=outs,
        in_specs=[pl.BlockSpec(memory_space=pltpu.SMEM)]
        + [hbm if i in hbm_ins else vmem for i in range(len(operands))],
        out_specs=tuple(hbm if i in hbm_outs else vmem for i in range(len(outs))),
        scratch_shapes=scratch,
        cost_estimate=pl.CostEstimate(flops=flops, bytes_accessed=12 << 20, transcendentals=0),
        compiler_params=pltpu.CompilerParams(vmem_limit_bytes=limit << 20),
    )(meta, *operands)


def same_core(subs):
    return [[s for s in range(subs) if s % 2 == core] for core in (0, 1)]


def locate(ids, position_of):
    identities = jnp.arange(position_of.shape[0], dtype=jnp.int32)
    return jnp.sum(jnp.where(ids[..., None] == identities, position_of, 0), axis=-1, dtype=jnp.int32)


def first_exchange(waves):
    copies = jnp.broadcast_to(waves, (lax.axis_size("sub"), *waves.shape))
    return lax.all_to_all(copies, "sub", split_axis=0, concat_axis=0, tiled=True)


def prepare_kernel(meta, located, everyone, state, injects, source, late, before, turned, row, sem):
    subs, ports, _ = everyone.shape
    cases, block = state.shape
    spacing = meta[1]
    start = spacing - 1
    load = pltpu.make_async_copy(source.at[start], row, sem)
    load.start()
    picked = jnp.zeros(before.shape, F32)
    for sub in range(subs):
        picked = jnp.where(located[...] == sub, everyone[sub].astype(F32), picked)
    before[...] = picked
    turned[:, :ports] = jnp.transpose(picked)
    waves = turned[pl.ds(pl.multiple_of(start * cases, cases), cases), :ports].astype(BF16)
    spread = jnp.where(port_rows(ports, block), 1.0, 0.0).astype(BF16)
    drive = injects[...] * jnp.dot(waves, spread, preferred_element_type=F32)
    load.wait()
    operand = state[...] + spacing.astype(F32) * (row[...].astype(F32) + drive)
    late[:ports, :] = picked.astype(BF16)
    late[ports:, :] = operand.astype(BF16)


def requests(partner, position_of):
    subs = lax.axis_size("sub")
    ports = partner.shape[0]
    ids = jnp.pad(partner.astype(BF16)[None, :], ((0, 15), (0, 128 - ports)))
    copies = jnp.broadcast_to(ids, (subs // 2, *ids.shape))
    everyone = lax.all_to_all(
        copies, "sub", split_axis=0, concat_axis=0, axis_index_groups=same_core(subs), tiled=True
    )
    return locate(everyone[:, 0, :ports].astype(jnp.int32), position_of)


def second_fetch(waves, located):
    subs = lax.axis_size("sub")
    sub = lax.axis_index("sub")
    swap = [(s * SLOTS + r, (s ^ 1) * SLOTS + r) for s in range(subs) for r in range(SLOTS)]
    others = lax.ppermute(waves, ("sub", "blk"), swap)
    wanted = located[:, :, None]
    zero = jnp.zeros((), BF16)
    sent = jnp.where(
        wanted == sub, waves[None], jnp.where(wanted == (sub ^ 1), others[None], zero)
    )
    parts = lax.all_to_all(
        sent, "sub", split_axis=0, concat_axis=0, axis_index_groups=same_core(subs), tiled=True
    )
    return jnp.sum(parts.astype(F32), axis=0)


def shards(initial_state, source, inverse_diag, inverse_off, coupling, initial_waves,
           bucket, partner, position_of):
    state, source, matrix = initial_state[0], source[0], inverse_off[0]
    steps, cases, block = source.shape
    nodes = matrix.shape[0]
    ports = coupling.shape[1]
    all_ports = SLOTS * ports
    x = lax.axis_index("blk")
    rel = lax.rem(x + 4 - 2 * lax.rem(lax.axis_index("sub"), 2), 4)

    count = jnp.where(bucket == 0, steps // 4, jnp.where(bucket == 1, steps // 2, steps))
    spacing = steps // count
    meta = jnp.concatenate([count, spacing, x[None]]).astype(jnp.int32)
    home_meta = jnp.concatenate([jnp.where(rel == 0, count, 1), meta[1:]])

    matrices = gather_matrix(matrix)
    injects = jnp.pad(coupling[0][:, None], ((0, 0), (0, block // ports - 1))).reshape(1, block)
    misc = jnp.concatenate([inverse_diag, injects, jnp.zeros((6, block), F32)], axis=0)
    miscs = to_home(misc)
    sources = to_home(source[1:])
    located = requests(partner[0], position_of)

    shape = jax.ShapeDtypeStruct
    everyone = first_exchange(initial_waves[0])
    column = jnp.broadcast_to(
        locate(partner[0], position_of)[:, None], (ports, steps * cases)
    )
    late, before = call(
        prepare_kernel,
        (shape((ports + cases, block), BF16), shape((ports, steps * cases), F32)),
        [pltpu.VMEM((steps * cases, 128), F32), pltpu.VMEM((cases, block), BF16),
         pltpu.SemaphoreType.DMA],
        4 << 20, 8, meta, column, everyone, state, injects, source, hbm_ins=(4,),
    )
    incoming = to_home(late)

    shape = jax.ShapeDtypeStruct
    slots, response, history = call(
        sweep_kernel,
        (shape((SLOTS, ports, steps * cases), BF16), shape((WIDE * steps * all_ports, nodes), BF16),
         shape((WIDE * steps * cases, nodes), F32)),
        [pltpu.VMEM((2, cases + all_ports, nodes), BF16), pltpu.VMEM((all_ports, nodes), F32),
         pltpu.VMEM((steps * cases, nodes), BF16), pltpu.VMEM((steps * all_ports, nodes), BF16),
         pltpu.VMEM((steps * cases, nodes), F32), pltpu.SemaphoreType.DMA((2, steps)),
         *(pltpu.VMEM(m.shape, BF16) for m in matrices), *(pltpu.VMEM(a.shape, BF16) for a in sources),
         pltpu.SemaphoreType.DMA((9,))],
        2 * steps * (cases + all_ports) * nodes * nodes, LIMITS[0], home_meta,
        *matrices, *sources, *miscs, *incoming, hbm_outs=(1, 2), hbm_ins=range(9),
    )
    at_ports, samples, last = call(
        ports_kernel,
        (shape((steps * all_ports, all_ports), BF16), shape((steps * cases, all_ports), F32),
         shape((cases, nodes), F32)),
        [pltpu.VMEM((steps * all_ports, nodes), BF16), pltpu.VMEM((steps * cases, nodes), F32),
         pltpu.SemaphoreType.DMA((2,))],
        2 * steps * (all_ports + 2 * cases) * nodes * all_ports, LIMITS[1], meta,
        response, history, hbm_ins=(0, 1),
    )

    waves = mine(from_home(slots), rel)
    after = second_fetch(waves, located)
    gain = spacing.astype(F32) * coupling[0]
    drives = turn((gain[:, None] * (after - before)).astype(BF16))
    (result,) = call(
        correct_whole,
        (shape((SLOTS, cases + ports, block), F32),),
        [pltpu.VMEM((2 * steps * cases, steps * all_ports), BF16),
         pltpu.VMEM((steps * cases, all_ports), F32),
         pltpu.VMEM((steps * all_ports, nodes), BF16), pltpu.SemaphoreType.DMA((4,))],
        2 * cases * steps * all_ports * nodes, LIMITS[2], meta,
        response, at_ports, samples, last, *drives, hbm_ins=(0,),
    )
    parts = from_home(result)
    last = mine(parts, rel, slice(0, cases))
    waveform = mine(parts, rel, slice(cases, None))
    return last[None], waveform[None]


LIMITS = (45, 45, 45)


def solution(mesh):
    return jax.shard_map(
        shards,
        mesh=mesh,
        in_specs=(
            P("sub", None, "blk"),
            P("sub", None, None, "blk"),
            P("sub", "blk"),
            P("sub", None, "blk"),
            P("sub", "blk"),
            P("sub", "blk", None),
            P("sub"),
            P("sub", "blk"),
            P(),
        ),
        out_specs=(P("sub", None, "blk"), P("sub", "blk", None)),
        check_vma=False,
    )
```

```python
import jax
import jax.numpy as jnp
from jax import lax
from jax.experimental import pallas as pl
from jax.experimental.pallas import tpu as pltpu
from jax.sharding import PartitionSpec as P


F32 = jnp.float32
BF16 = jnp.bfloat16
SLOTS = 4
FAR_ROWS = 1280
WIDE = 5


def hop(array, start, end):
    pairs = []
    for sub in range(32):
        home = 2 * (sub % 2)
        pairs.append((sub * 4 + (home + start) % 4, sub * 4 + (home + end) % 4))
    return lax.ppermute(array, ("sub", "blk"), pairs)


def to_home(array):
    return array, *(hop(array, d, 0) for d in (1, 2, 3))


def turn(array):
    parts = [array]
    for d in (1, 2, 3):
        pairs = [(sub * 4 + (r + d) % 4, sub * 4 + r) for sub in range(32) for r in range(4)]
        parts.append(lax.ppermute(array, ("sub", "blk"), pairs))
    return tuple(parts)


def from_home(slots):
    return slots[0], *(hop(slots[d], 0, d) for d in (1, 2, 3))


def mine(parts, rel, rows=slice(None)):
    zero, one, two, three = (part[rows] for part in parts)
    return jnp.where(rel == 0, zero, jnp.where(rel == 1, one, jnp.where(rel == 2, two, three)))


def gather_matrix(matrix):
    half = FAR_ROWS
    one, three = hop(matrix, 1, 0), hop(matrix, 3, 0)
    near1, near3 = hop(matrix[:half], 2, 1), hop(matrix[half:], 2, 3)
    upper, lower = hop(near1, 1, 0), hop(near3, 3, 0)
    return matrix, one, upper, lower, three


def port_rows(ports, nodes):
    stride = nodes // ports
    port_at = lax.broadcasted_iota(jnp.int32, (ports, nodes), 0) * stride
    node_at = lax.broadcasted_iota(jnp.int32, (ports, nodes), 1)
    return port_at == node_at


def port_columns(ports, nodes):
    stride = nodes // ports
    port_at = lax.broadcasted_iota(jnp.int32, (nodes, ports), 1) * stride
    node_at = lax.broadcasted_iota(jnp.int32, (nodes, ports), 0)
    return port_at == node_at


def times_matrix(operand, matrices, d):
    if d == 2:
        half = FAR_ROWS
        total = jnp.dot(operand[:, :half], matrices[2][...], preferred_element_type=F32)
        return total + jnp.dot(operand[:, half:], matrices[3][...], preferred_element_type=F32)
    matrix = matrices[{0: 0, 1: 1, 3: 4}[d]]
    return jnp.dot(operand[...], matrix[...], preferred_element_type=F32)


DIAG = 0
INJECT = 1


def sweep_kernel(meta, a0_in, a1_in, a2_in, a3_in, a4_in, s0_in, s1_in, s2_in, s3_in, m0, m1, m2, m3, w0, w1, w2, w3,
                 out, response_out, history_out, operand, state, forced, response, history,
                 sent, a0, a1, a2, a3, a4, s0, s1, s2, s3, arrived):
    later_steps, cases, block = s0.shape
    steps = later_steps + 1
    ports = w0.shape[0] - cases
    all_ports = SLOTS * ports
    nodes = SLOTS * block
    count, spacing, place = meta[0], meta[1], meta[2]
    spacing_float = spacing.astype(F32)
    matrices, sources, miscs = (a0, a1, a2, a3, a4), (s0, s1, s2, s3), (m0, m1, m2, m3)
    inputs = (s0_in, s1_in, s2_in, s3_in, a0_in, a1_in, a2_in, a3_in, a4_in)
    loads = [
        pltpu.make_async_copy(here, there, arrived.at[i])
        for i, (here, there) in enumerate(zip(inputs, sources + matrices))
    ]
    for load in loads:
        load.start()
    marks = port_rows(all_ports, nodes)
    spread = jnp.where(marks, 1.0, 0.0).astype(BF16)
    waves = jnp.concatenate([w[:ports, :] for w in (w0, w1, w2, w3)], axis=0).astype(F32)
    waves = jnp.transpose(waves).astype(BF16)
    forced[...] = jnp.dot(waves, spread, preferred_element_type=F32).astype(BF16)
    state[...] = jnp.where(marks, 1.0, 0.0)

    def argument(current, fine, d):
        rows = pl.ds(pl.multiple_of(fine * cases, cases), cases)
        lanes = slice(d * block, (d + 1) * block)
        drive = miscs[d][INJECT : INJECT + 1, :] * forced[rows, lanes].astype(F32)
        return (current + spacing_float * (sources[d][fine - 1].astype(F32) + drive)).astype(BF16)

    def spot(d):
        return pl.ds(pl.multiple_of(lax.rem(place + d, SLOTS) * block, block), block)

    for d, late in enumerate((w0, w1, w2, w3)):
        operand[0, :cases, spot(d)] = late[ports:, :]
        operand[0, cases:, spot(d)] = spread[:, d * block : (d + 1) * block]

    def send(k):
        rows = pl.ds(pl.multiple_of(k * all_ports, all_ports), all_ports)
        held = pl.ds(pl.multiple_of(k * cases, cases), cases)
        return (
            pltpu.make_async_copy(response.at[rows, :], response_out.at[rows, :], sent.at[0, k]),
            pltpu.make_async_copy(history.at[held, :], history_out.at[held, :], sent.at[1, k]),
        )

    def step(k, carry):
        now, later = lax.rem(k, 2), lax.rem(k + 1, 2)
        fine = jnp.minimum((k + 2) * spacing - 1, steps - 1)
        held = pl.ds(pl.multiple_of(k * cases, cases), cases)
        rows = pl.ds(pl.multiple_of(k * all_ports, all_ports), all_ports)
        for d in range(SLOTS):
            lanes = slice(d * block, (d + 1) * block)
            if carry is None:
                for load in {0: loads[4:5], 1: loads[5:6], 2: loads[6:8], 3: loads[8:]}[d]:
                    load.wait()
            total = times_matrix(operand.at[now], matrices, d)
            diag = miscs[d][DIAG : DIAG + 1, :]
            new = total[:cases] + diag * operand[now, :cases, spot(d)].astype(F32)
            history[held, lanes] = new
            operand[later, :cases, spot(d)] = argument(new, fine, d)
            reply = total[cases:] + diag * state[:, lanes]
            state[:, lanes] = reply
            response[rows, lanes] = reply.astype(BF16)
            operand[later, cases:, spot(d)] = reply.astype(BF16)
        for copy in send(k):
            copy.start()
        return carry

    for load in loads[:SLOTS]:
        load.wait()
    step(jnp.int32(0), None)
    lax.fori_loop(1, count, step, 0)

    def clear(p, carry):
        rows = pl.ds(pl.multiple_of(p * all_ports, all_ports), all_ports)
        response[rows, :] = jnp.zeros((all_ports, nodes), BF16)
        held = pl.ds(pl.multiple_of(p * cases, cases), cases)
        history[held, :] = jnp.zeros((cases, nodes), F32)
        for copy in send(p):
            copy.start()
        return carry

    lax.fori_loop(count, steps, clear, 0)
    pick = jnp.where(port_columns(all_ports, nodes), 1.0, 0.0).astype(BF16)
    coarse = jnp.dot(history[...].astype(BF16), pick, preferred_element_type=F32)
    forced[: steps * cases, :all_ports] = coarse.astype(BF16)
    pieces = []
    for g in range(steps):
        at = lax.div(jnp.int32(g), spacing) * cases
        rows = pl.ds(pl.multiple_of(at, cases), cases)
        pieces.append(forced[rows, :all_ports].astype(F32))
    wave = jnp.transpose(jnp.concatenate(pieces, axis=0))
    for d in range(SLOTS):
        out[d] = wave[d * ports : (d + 1) * ports].astype(BF16)
    for p in range(steps):
        for copy in send(p):
            copy.wait()


def ports_kernel(meta, response_in, history_in, at_ports, samples, last, response, history,
                 arrived):
    nodes = history.shape[1]
    all_ports = at_ports.shape[1]
    steps = response.shape[0] // all_ports
    cases = history.shape[0] // steps
    first = pltpu.make_async_copy(history_in.at[: steps * cases, :], history, arrived.at[0])
    second = pltpu.make_async_copy(
        response_in.at[: steps * all_ports, :], response, arrived.at[1]
    )
    first.start()
    second.start()
    pick = jnp.where(port_columns(all_ports, nodes), 1.0, 0.0).astype(BF16)
    first.wait()
    high = history[...].astype(BF16)
    low = (history[...] - high.astype(F32)).astype(BF16)
    samples[...] = jnp.dot(high, pick, preferred_element_type=F32)
    samples[...] += jnp.dot(low, pick, preferred_element_type=F32)
    second.wait()
    at_ports[...] = jnp.dot(response[...], pick, preferred_element_type=F32).astype(BF16)
    last[...] = history[pl.ds(pl.multiple_of((meta[0] - 1) * cases, cases), cases), :]


def correct_kernel(meta, response_in, at_ports, last, v0, v1, v2, v3, out, toeplitz,
                   response, arrived):
    cases, nodes = last.shape
    ports, fine_cases = v0.shape
    steps = fine_cases // cases
    block = nodes // SLOTS
    all_ports = SLOTS * ports
    count, spacing = meta[0], meta[1]
    pieces = 4
    part = response.shape[0] // pieces
    copies = []
    for i in range(pieces):
        rows = pl.ds(i * part, part)
        copies.append(
            pltpu.make_async_copy(response_in.at[rows, :], response.at[rows, :], arrived.at[i])
        )
        copies[-1].start()
    drive = jnp.concatenate([v[...] for v in (v0, v1, v2, v3)], axis=0).astype(F32)
    samples_at = jnp.transpose(drive).astype(BF16)
    scratch = toeplitz.at[pl.ds(steps * cases, fine_cases), pl.ds(0, all_ports)]
    scratch[...] = samples_at
    zero = jnp.zeros((cases, all_ports), BF16)
    for i in range(steps):
        fine = jnp.minimum((i + 1) * spacing - 1, steps - 1)
        driven = scratch[pl.ds(pl.multiple_of(fine * cases, cases), cases), :]
        for k in range(i, steps):
            lag = k - i
            toeplitz[k * cases : (k + 1) * cases, lag * all_ports : (lag + 1) * all_ports] = driven
        for lag in range(i + 1, steps):
            toeplitz[i * cases : (i + 1) * cases, lag * all_ports : (lag + 1) * all_ports] = zero
    moved = jnp.dot(toeplitz[: steps * cases, :], at_ports[...], preferred_element_type=F32)
    toe_rows = pl.ds(pl.multiple_of((count - 1) * cases, cases), cases)
    total = last[...]
    for i, copy in enumerate(copies):
        copy.wait()
        rows = slice(i * part, (i + 1) * part)
        total += jnp.dot(toeplitz[toe_rows, rows], response[rows, :], preferred_element_type=F32)
    for d in range(SLOTS):
        out[d, :cases, :] = total[:, d * block : (d + 1) * block]
    return moved


def correct_whole(meta, response, at_ports, samples, last, v0, v1, v2, v3, out, toeplitz, held,
                  response_in, arrived):
    cases = last.shape[0]
    ports, fine_cases = v0.shape
    held[...] = samples[...] + correct_kernel(
        meta, response, at_ports, last, v0, v1, v2, v3, out, toeplitz, response_in, arrived
    )
    pieces = []
    for g in range(fine_cases // cases):
        at = lax.div(jnp.int32(g), meta[1]) * cases
        pieces.append(held[pl.ds(pl.multiple_of(at, cases), cases), :])
    wave = jnp.transpose(jnp.concatenate(pieces, axis=0))
    for d in range(SLOTS):
        out[d, cases:, :] = wave[d * ports : (d + 1) * ports]


def choose_kernel(rel, home, one, two, three, last, waveform, sent):
    cases, rows = last.shape[0], one.shape[0]
    for d, part in enumerate((home.at[0], one, two, three)):

        @pl.when(rel[0] == d)
        def _(part=part):
            copies = (
                pltpu.make_async_copy(part.at[pl.ds(0, cases), :], last, sent.at[0]),
                pltpu.make_async_copy(part.at[pl.ds(cases, rows - cases), :], waveform, sent.at[1]),
            )
            for copy in copies:
                copy.start()
            for copy in copies:
                copy.wait()


def call(kernel, outs, scratch, flops, limit, meta, *operands, hbm_outs=(), hbm_ins=()):
    vmem, hbm = pl.BlockSpec(memory_space=pltpu.VMEM), pl.BlockSpec(memory_space=pltpu.HBM)
    outs = tuple(outs)
    return pl.pallas_call(
        kernel,
        out_shape=outs,
        in_specs=[pl.BlockSpec(memory_space=pltpu.SMEM)]
        + [hbm if i in hbm_ins else vmem for i in range(len(operands))],
        out_specs=tuple(hbm if i in hbm_outs else vmem for i in range(len(outs))),
        scratch_shapes=scratch,
        cost_estimate=pl.CostEstimate(flops=flops, bytes_accessed=12 << 20, transcendentals=0),
        compiler_params=pltpu.CompilerParams(vmem_limit_bytes=limit << 20),
    )(meta, *operands)


def same_core(subs):
    return [[s for s in range(subs) if s % 2 == core] for core in (0, 1)]


def locate(ids, position_of):
    identities = jnp.arange(position_of.shape[0], dtype=jnp.int32)
    return jnp.sum(jnp.where(ids[..., None] == identities, position_of, 0), axis=-1, dtype=jnp.int32)


def first_exchange(waves):
    copies = jnp.broadcast_to(waves, (lax.axis_size("sub"), *waves.shape))
    return lax.all_to_all(copies, "sub", split_axis=0, concat_axis=0, tiled=True)


def prepare_kernel(meta, located, everyone, state, injects, source, late, before, turned, row, sem):
    subs, ports, _ = everyone.shape
    cases, block = state.shape
    spacing = meta[1]
    start = spacing - 1
    load = pltpu.make_async_copy(source.at[start], row, sem)
    load.start()
    picked = jnp.zeros(before.shape, F32)
    for sub in range(subs):
        picked = jnp.where(located[...] == sub, everyone[sub].astype(F32), picked)
    before[...] = picked
    turned[:, :ports] = jnp.transpose(picked)
    waves = turned[pl.ds(pl.multiple_of(start * cases, cases), cases), :ports].astype(BF16)
    spread = jnp.where(port_rows(ports, block), 1.0, 0.0).astype(BF16)
    drive = injects[...] * jnp.dot(waves, spread, preferred_element_type=F32)
    load.wait()
    operand = state[...] + spacing.astype(F32) * (row[...].astype(F32) + drive)
    late[:ports, :] = picked.astype(BF16)
    late[ports:, :] = operand.astype(BF16)


def requests(partner, position_of):
    subs = lax.axis_size("sub")
    ports = partner.shape[0]
    ids = jnp.pad(partner.astype(BF16)[None, :], ((0, 15), (0, 128 - ports)))
    copies = jnp.broadcast_to(ids, (subs // 2, *ids.shape))
    everyone = lax.all_to_all(
        copies, "sub", split_axis=0, concat_axis=0, axis_index_groups=same_core(subs), tiled=True
    )
    return locate(everyone[:, 0, :ports].astype(jnp.int32), position_of)


def second_fetch(waves, located):
    subs = lax.axis_size("sub")
    sub = lax.axis_index("sub")
    swap = [(s * SLOTS + r, (s ^ 1) * SLOTS + r) for s in range(subs) for r in range(SLOTS)]
    others = lax.ppermute(waves, ("sub", "blk"), swap)
    wanted = located[:, :, None]
    zero = jnp.zeros((), BF16)
    sent = jnp.where(
        wanted == sub, waves[None], jnp.where(wanted == (sub ^ 1), others[None], zero)
    )
    parts = lax.all_to_all(
        sent, "sub", split_axis=0, concat_axis=0, axis_index_groups=same_core(subs), tiled=True
    )
    return jnp.sum(parts.astype(F32), axis=0)


def shards(initial_state, source, inverse_diag, inverse_off, coupling, initial_waves,
           bucket, partner, position_of):
    state, source, matrix = initial_state[0], source[0], inverse_off[0]
    steps, cases, block = source.shape
    nodes = matrix.shape[0]
    ports = coupling.shape[1]
    all_ports = SLOTS * ports
    x = lax.axis_index("blk")
    rel = lax.rem(x + 4 - 2 * lax.rem(lax.axis_index("sub"), 2), 4)

    count = jnp.where(bucket == 0, steps // 4, jnp.where(bucket == 1, steps // 2, steps))
    spacing = steps // count
    meta = jnp.concatenate([count, spacing, x[None]]).astype(jnp.int32)
    home_meta = jnp.concatenate([jnp.where(rel == 0, count, 1), meta[1:]])

    matrices = gather_matrix(matrix)
    injects = jnp.pad(coupling[0][:, None], ((0, 0), (0, block // ports - 1))).reshape(1, block)
    misc = jnp.concatenate([inverse_diag, injects, jnp.zeros((6, block), F32)], axis=0)
    miscs = to_home(misc)
    sources = to_home(source[1:])
    located = requests(partner[0], position_of)

    shape = jax.ShapeDtypeStruct
    everyone = first_exchange(initial_waves[0])
    column = jnp.broadcast_to(
        locate(partner[0], position_of)[:, None], (ports, steps * cases)
    )
    late, before = call(
        prepare_kernel,
        (shape((ports + cases, block), BF16), shape((ports, steps * cases), F32)),
        [pltpu.VMEM((steps * cases, 128), F32), pltpu.VMEM((cases, block), BF16),
         pltpu.SemaphoreType.DMA],
        4 << 20, 8, meta, column, everyone, state, injects, source, hbm_ins=(4,),
    )
    incoming = to_home(late)

    shape = jax.ShapeDtypeStruct
    slots, response, history = call(
        sweep_kernel,
        (shape((SLOTS, ports, steps * cases), BF16), shape((WIDE * steps * all_ports, nodes), BF16),
         shape((WIDE * steps * cases, nodes), F32)),
        [pltpu.VMEM((2, cases + all_ports, nodes), BF16), pltpu.VMEM((all_ports, nodes), F32),
         pltpu.VMEM((steps * cases, nodes), BF16), pltpu.VMEM((steps * all_ports, nodes), BF16),
         pltpu.VMEM((steps * cases, nodes), F32), pltpu.SemaphoreType.DMA((2, steps)),
         *(pltpu.VMEM(m.shape, BF16) for m in matrices), *(pltpu.VMEM(a.shape, BF16) for a in sources),
         pltpu.SemaphoreType.DMA((9,))],
        2 * steps * (cases + all_ports) * nodes * nodes, LIMITS[0], home_meta,
        *matrices, *sources, *miscs, *incoming, hbm_outs=(1, 2), hbm_ins=range(9),
    )
    at_ports, samples, last = call(
        ports_kernel,
        (shape((steps * all_ports, all_ports), BF16), shape((steps * cases, all_ports), F32),
         shape((cases, nodes), F32)),
        [pltpu.VMEM((steps * all_ports, nodes), BF16), pltpu.VMEM((steps * cases, nodes), F32),
         pltpu.SemaphoreType.DMA((2,))],
        2 * steps * (all_ports + 2 * cases) * nodes * all_ports, LIMITS[1], meta,
        response, history, hbm_ins=(0, 1),
    )

    waves = mine(from_home(slots), rel)
    after = second_fetch(waves, located)
    gain = spacing.astype(F32) * coupling[0]
    drives = turn((gain[:, None] * (after - before)).astype(BF16))
    (result,) = call(
        correct_whole,
        (shape((SLOTS, cases + ports, block), F32),),
        [pltpu.VMEM((2 * steps * cases, steps * all_ports), BF16),
         pltpu.VMEM((steps * cases, all_ports), F32),
         pltpu.VMEM((steps * all_ports, nodes), BF16), pltpu.SemaphoreType.DMA((4,))],
        2 * cases * steps * all_ports * nodes, LIMITS[2], meta,
        response, at_ports, samples, last, *drives, hbm_ins=(0,),
    )
    parts = (result, *from_home(result)[1:])
    last, waveform = call(
        choose_kernel,
        (shape((cases, block), F32), shape((ports, steps * cases), F32)),
        [pltpu.SemaphoreType.DMA((2,))], 1 << 20, 8, rel.astype(jnp.int32)[None], *parts,
        hbm_outs=(0, 1),
    )
    return last[None], waveform[None]


LIMITS = (45, 45, 45)


def solution(mesh):
    return jax.shard_map(
        shards,
        mesh=mesh,
        in_specs=(
            P("sub", None, "blk"),
            P("sub", None, None, "blk"),
            P("sub", "blk"),
            P("sub", None, "blk"),
            P("sub", "blk"),
            P("sub", "blk", None),
            P("sub"),
            P("sub", "blk"),
            P(),
        ),
        out_specs=(P("sub", None, "blk"), P("sub", "blk", None)),
        check_vma=False,
    )
```
